128 devices in a mesh: group: 8 (over y, x_hi), head: 8 (over z, x_lo), seq: 2 (over core).
Axes of the slice: x: 4 (x_hi: 2, x_lo: 2; x = x_hi * 2 + x_lo), y: 4, z: 4, core: 2. Of those that a mesh axis runs over, the one named last changes fastest.
Arguments:
- prefix_q: bfloat16 [3072, 4096], P(('group', 'seq'), 'head'), may hold values from -32 to 32
- prefix_k: bfloat16 [3072, 1024], P(('group', 'seq'), 'head'), may hold values from -6 to 6
- prefix_v: bfloat16 [3072, 1024], P(('group', 'seq'), 'head'), may hold values from -6 to 6
- resp_q: bfloat16 [8192, 4096], P(('group', 'seq'), 'head'), may hold values from -32 to 32
- resp_k: bfloat16 [8192, 1024], P(('group', 'seq'), 'head'), may hold values from -6 to 6
- resp_v: bfloat16 [8192, 1024], P(('group', 'seq'), 'head'), may hold values from -6 to 6
- resp_len: int32 [16], P(('group', 'seq')), may hold values from 64 to 512
- resp_prompt: int32 [16], P(('group', 'seq')), may hold values from 0 to 1
- out_weight: bfloat16 [4096, 4096], P('head'), may hold values from -0.09375 to 0.09375
- prefix_grad: bfloat16 [3072, 4096], P(('group', 'seq'), 'head'), may hold values from -6 to 6
- resp_grad: bfloat16 [8192, 4096], P(('group', 'seq'), 'head'), may hold values from -6 to 6
Outputs:
- prefix_out: bfloat16 [3072, 4096], P(('group', 'seq'), 'head')
- resp_out: bfloat16 [8192, 4096], P(('group', 'seq'), 'head')
- d_prefix_q: bfloat16 [3072, 4096], P(('group', 'seq'), 'head')
- d_prefix_k: bfloat16 [3072, 1024], P(('group', 'seq'), 'head')
- d_prefix_v: bfloat16 [3072, 1024], P(('group', 'seq'), 'head')
- d_resp_q: bfloat16 [8192, 4096], P(('group', 'seq'), 'head')
- d_resp_k: bfloat16 [8192, 1024], P(('group', 'seq'), 'head')
- d_resp_v: bfloat16 [8192, 1024], P(('group', 'seq'), 'head')
- d_out_weight: float32 [4096, 4096], P('head')
The draws below stay inside these ranges and needn't reach their ends.
Inputs may be any that keep to these rules, and one draw needn't show every extreme that they name: Rows from resp_len to 512 of a response slot are padding.
All inputs are finite; a program needn't handle non-finite values.
Results may differ from the reference program's by a relative error of at most 0.017.
Values may be sent and summed in bfloat16 or wider, within the bound.
No kernel may reach another device: no remote copies, remote signals or barrier semaphores. Data moves between devices by JAX's collectives and lax.ppermute only.
A program may use at most 192 MiB of HBM per device.

```python
import jax
import jax.numpy as jnp
from jax import lax

D = 4096
QH = 32
KVH = 8
HD = 128
RMAX = 512
PREFIX = 3072
RESP = 16


def drawn_rows(key, salt, rows, heads):
    base = jnp.clip(jax.random.normal(jax.random.fold_in(key, salt), (rows, heads * HD), jnp.float32), -6.0, 6.0)
    return base


def draw_prefix_q(key, part):
    return drawn_rows(key, 101, PREFIX, QH).astype(jnp.bfloat16)


def draw_resp_q(key, part):
    return drawn_rows(key, 202, RESP * RMAX, QH).astype(jnp.bfloat16)


def draw_prefix_k(key, part):
    return drawn_rows(key, 303, PREFIX, KVH).astype(jnp.bfloat16)


def set_ends(values, stream_key, low, top_value):
    longest = values.shape.index(max(values.shape))
    spots = []
    for shift in (0, 1):
        where = [jax.random.randint(jax.random.fold_in(stream_key, axis), (), 0, length) for axis, length in enumerate(values.shape)]
        where[longest] = (where[longest] + shift) % values.shape[longest]
        spots.append(tuple(where))
    return values.at[spots[0]].set(low).at[spots[1]].set(top_value)


def block_scale(key, dims, split, smallest, top_value):
    gain = 1.0
    for axis_at, blocks in split:
        steps = jax.random.uniform(jax.random.fold_in(jax.random.fold_in(key, 6), axis_at), (blocks,), jnp.float32, smallest / len(split), top_value / len(split))
        gain = gain * jnp.repeat(jnp.exp(steps), dims[axis_at] // blocks).reshape((-1,) + (1,) * (len(dims) - 1 - axis_at))
    return gain


def normal_values(key, shape, scale, bound, shards=(), held_as=jnp.bfloat16):
    result = scale * jax.random.normal(key, shape, jnp.float32)
    if shards:
        result = result * block_scale(key, shape, shards, -0.22, 0.18)
    return jnp.clip(result, -bound, bound).astype(held_as)


def setup_inputs(seed: int = 0) -> dict:
    splits = jax.random.split(jax.random.key(seed), 12)
    prefix_q = draw_prefix_q(jax.random.fold_in(splits[11], 71), 0)
    prefix_k = draw_prefix_k(jax.random.fold_in(splits[11], 71), 0)
    prefix_v = normal_values(splits[2], (PREFIX, KVH * HD), 1.0, 6.0, ((0, 16), (1, 8)))
    resp_q = draw_resp_q(jax.random.fold_in(splits[11], 71), 0)
    resp_k = normal_values(splits[4], (RESP * RMAX, KVH * HD), 1.0, 6.0, ((0, 16), (1, 8)))
    resp_v = normal_values(splits[5], (RESP * RMAX, KVH * HD), 1.0, 6.0, ((0, 16), (1, 8)))
    resp_len = set_ends(jax.random.randint(splits[6], (RESP,), RMAX // 8, RMAX + 1), jax.random.fold_in(splits[6], 1), RMAX // 8, RMAX).astype(jnp.int32)
    resp_prompt = set_ends(jax.random.randint(splits[7], (RESP,), 0, 2), jax.random.fold_in(splits[7], 1), 0, 1).astype(jnp.int32)
    out_weight = normal_values(splits[8], (QH * HD, D), (QH * HD) ** -0.5, 0.09375, ((0, 8),))
    prefix_grad = normal_values(splits[9], (PREFIX, D), 1.0, 6.0, ((0, 16), (1, 8)))
    resp_grad = normal_values(splits[10], (RESP * RMAX, D), 1.0, 6.0, ((0, 16), (1, 8)))
    return {"prefix_q": prefix_q, "prefix_k": prefix_k, "prefix_v": prefix_v, "resp_q": resp_q, "resp_k": resp_k, "resp_v": resp_v, "resp_len": resp_len, "resp_prompt": resp_prompt, "out_weight": out_weight, "prefix_grad": prefix_grad, "resp_grad": resp_grad}


masked_value = -1e30


def rounded(value):
    return lax.optimization_barrier(value.astype(jnp.bfloat16)).astype(jnp.float32)


def attend(queries, keys, values, seen, dout, valid):
    scale = HD ** -0.5
    highest = lax.Precision.HIGHEST
    raw = jnp.einsum("brgd,bnd->bgrn", queries, keys, precision=highest) * scale
    scores = jnp.where(seen[:, None], raw, masked_value)
    top = jnp.max(scores, -1, keepdims=True)
    lse = top + jnp.log(jnp.sum(jnp.exp(scores - top), -1, keepdims=True))
    prob = jnp.exp(scores - lse)
    weights = rounded(prob)
    heads_out = rounded(jnp.einsum("bgrn,bnd->brgd", weights, values, precision=highest) * valid[:, :, None, None])
    delta = jnp.transpose(jnp.sum(dout * heads_out, -1), (0, 2, 1))
    dprob = jnp.einsum("brgd,bnd->bgrn", dout, values, precision=highest)
    dscore = rounded(prob * (dprob - delta[..., None]))
    dquery = jnp.einsum("bgrn,bnd->brgd", dscore, keys, precision=highest)
    dkey = jnp.einsum("bgrn,brgd->bnd", dscore, queries, precision=highest)
    dvalue = jnp.einsum("bgrn,brgd->bnd", weights, dout, precision=highest)
    return heads_out, dquery, dkey, dvalue


def reference(prefix_q, prefix_k, prefix_v, resp_q, resp_k, resp_v, resp_len, resp_prompt, out_weight, prefix_grad, resp_grad):
    group_q = QH // KVH
    prompt_len = PREFIX // 2
    scale = HD ** -0.5
    highest = lax.Precision.HIGHEST
    live = (jnp.arange(RMAX, dtype=jnp.int32)[None, :] < resp_len[:, None]).astype(jnp.float32)
    live_rows = live.reshape(RESP * RMAX)
    pq = prefix_q.astype(jnp.float32).reshape(2, prompt_len, KVH, group_q, HD).transpose(2, 0, 1, 3, 4)
    pk = prefix_k.astype(jnp.float32).reshape(2, prompt_len, KVH, HD).transpose(2, 0, 1, 3)
    pv = prefix_v.astype(jnp.float32).reshape(2, prompt_len, KVH, HD).transpose(2, 0, 1, 3)
    rq = resp_q.astype(jnp.float32).reshape(RESP, RMAX, KVH, group_q, HD).transpose(2, 0, 1, 3, 4)
    rk = resp_k.astype(jnp.float32).reshape(RESP, RMAX, KVH, HD).transpose(2, 0, 1, 3)
    rv = resp_v.astype(jnp.float32).reshape(RESP, RMAX, KVH, HD).transpose(2, 0, 1, 3)
    wo = out_weight.reshape(KVH, group_q * HD, D)
    causal = jnp.arange(prompt_len)[:, None] >= jnp.arange(prompt_len)[None, :]
    self_causal = jnp.arange(RMAX)[:, None] >= jnp.arange(RMAX)[None, :]
    resp_seen = jnp.concatenate([jnp.ones((RMAX, prompt_len), bool), self_causal], 1)
    chosen = (resp_prompt[None, :] == jnp.arange(2, dtype=jnp.int32)[:, None]).astype(jnp.float32)

    def per_head(inputs):
        wo_h, pq_h, pk_h, pv_h, rq_h, rk_h, rv_h = inputs
        dout_p = rounded(jnp.dot(prefix_grad, wo_h.T, preferred_element_type=jnp.float32))
        dout_p = dout_p.reshape(2, prompt_len, group_q, HD)
        dout_r = rounded(jnp.dot(resp_grad, wo_h.T, preferred_element_type=jnp.float32) * live_rows[:, None])
        dout_r = dout_r.reshape(RESP, RMAX, group_q, HD)
        out_p, dq_p, dk_p, dv_p = attend(pq_h, pk_h, pv_h, causal[None], dout_p, jnp.ones((2, prompt_len), jnp.float32))
        keys = jnp.concatenate([pk_h[resp_prompt], rk_h], 1)
        values = jnp.concatenate([pv_h[resp_prompt], rv_h], 1)
        out_r, dq_r, dk_r, dv_r = attend(rq_h, keys, values, resp_seen[None], dout_r, live)
        dk_p = dk_p + jnp.einsum("pb,bnd->pnd", chosen, dk_r[:, :prompt_len], precision=highest)
        dv_p = dv_p + jnp.einsum("pb,bnd->pnd", chosen, dv_r[:, :prompt_len], precision=highest)
        return out_p, out_r, dq_p, dq_r, dk_p, dv_p, dk_r[:, prompt_len:], dv_r[:, prompt_len:]

    out_p, out_r, dq_p, dq_r, dk_p, dv_p, dk_r, dv_r = lax.map(per_head, (wo, pq, pk, pv, rq, rk, rv))
    attn_p = out_p.transpose(1, 2, 0, 3, 4).reshape(PREFIX, QH * HD).astype(jnp.bfloat16)
    attn_r = out_r.transpose(1, 2, 0, 3, 4).reshape(RESP * RMAX, QH * HD).astype(jnp.bfloat16)
    prefix_out = jnp.dot(attn_p, out_weight, preferred_element_type=jnp.float32).astype(jnp.bfloat16)
    resp_out = jnp.dot(attn_r, out_weight, preferred_element_type=jnp.float32).astype(jnp.bfloat16)
    weight_grad = jnp.dot(attn_p.T, prefix_grad, preferred_element_type=jnp.float32)
    weight_grad = weight_grad + jnp.dot(attn_r.T, resp_grad, preferred_element_type=jnp.float32)
    d_prefix_q = (dq_p * scale).transpose(1, 2, 0, 3, 4).reshape(PREFIX, QH * HD).astype(jnp.bfloat16)
    d_resp_q = (dq_r * scale).transpose(1, 2, 0, 3, 4).reshape(RESP * RMAX, QH * HD).astype(jnp.bfloat16)
    d_prefix_k = (dk_p * scale).transpose(1, 2, 0, 3).reshape(PREFIX, KVH * HD).astype(jnp.bfloat16)
    d_prefix_v = dv_p.transpose(1, 2, 0, 3).reshape(PREFIX, KVH * HD).astype(jnp.bfloat16)
    d_resp_k = (dk_r * scale).transpose(1, 2, 0, 3).reshape(RESP * RMAX, KVH * HD).astype(jnp.bfloat16)
    d_resp_v = dv_r.transpose(1, 2, 0, 3).reshape(RESP * RMAX, KVH * HD).astype(jnp.bfloat16)
    return (prefix_out, resp_out, d_prefix_q, d_prefix_k, d_prefix_v, d_resp_q, d_resp_k, d_resp_v, weight_grad)
```

```python
import jax
import jax.numpy as jnp
from jax import lax
from jax.experimental import pallas as pl
from jax.experimental.pallas import tpu as pltpu
from jax.sharding import PartitionSpec as P

HD = 128
RMAX = 512
HEADS = 4
SCALE = HD ** -0.5
C2 = SCALE * 1.4426950408889634
LN2 = 0.6931471805599453
MASKED = -1e30
RB = 128
PB = 96
F32 = jnp.float32
BF16 = jnp.bfloat16


def nt(a, b):
    return lax.dot_general(a, b, (((1,), (1,)), ((), ())), preferred_element_type=F32)


def nn(a, b):
    return jnp.dot(a, b, preferred_element_type=F32)


def tn(a, b):
    return lax.dot_general(a, b, (((0,), (0,)), ((), ())), preferred_element_type=F32)


def stacked(ref, start, rows):
    return jnp.concatenate(
        [ref[pl.ds(start, rows), h * HD : (h + 1) * HD] for h in range(HEADS)], 0
    )


def three_parts(column):
    hi = column.astype(BF16)
    rest = column - hi.astype(F32)
    mid = rest.astype(BF16)
    low = (rest - mid.astype(F32)).astype(BF16)
    lane = lax.broadcasted_iota(jnp.int32, (column.shape[0], HD), 1)
    out = jnp.where(lane == 2, low.astype(F32), 0.0)
    out = jnp.where(lane == 1, mid.astype(F32), out)
    out = jnp.where(lane == 0, hi.astype(F32), out)
    return out.astype(BF16)


def attend_block(q, pieces):
    scores = []
    for k, _, seen in pieces:
        s = nt(q, k)
        if seen is not None:
            s = jnp.where(seen, s, MASKED)
        scores.append(s)
    top = jnp.max(scores[0], 1, keepdims=True)
    for s in scores[1:]:
        top = jnp.maximum(top, jnp.max(s, 1, keepdims=True))
    acc = jnp.zeros((q.shape[0], 2 * HD), F32)
    for s, (_, v, _) in zip(scores, pieces):
        p = jnp.exp2((s - top) * C2).astype(BF16)
        acc += nn(p, jnp.concatenate([v, jnp.ones(v.shape, BF16)], 1))
    total = acc[:, HD : HD + 1]
    out = acc[:, :HD] / total
    return out, -(top + jnp.log(total) * (1.0 / SCALE))


def put_heads(out_ref, start, rows, out):
    for h in range(HEADS):
        out_ref[pl.ds(start, rows), h * HD : (h + 1) * HD] = out[h * rows : (h + 1) * rows].astype(
            BF16
        )


def fwd_kernel(info, pq, rq, near, far, rk, rv, attn, nl, kv):
    my_base = pl.multiple_of(info[0], 512)
    my_row = info[1]
    base = pl.multiple_of(info[2], 512)
    length = info[3]
    y, xh, c = info[4], info[5], info[6]
    shard = near.shape[2]
    prompt_len = kv.shape[0] // 2
    pref_rows = pq.shape[0]
    for m, ref in enumerate((near, far)):
        for k in range(4):
            for j in range(2):
                at = ((y ^ k) * 2 + (xh ^ j)) * 2 + (c ^ m)
                kv[pl.ds(pl.multiple_of(at * shard, shard), shard), :] = ref[k, j]

    def pref_body(i, _):
        start = pl.multiple_of(i * PB, PB)
        q = stacked(pq, start, PB)
        k = kv[pl.ds(my_base, prompt_len), :HD]
        v = kv[pl.ds(my_base, prompt_len), HD:]
        row = lax.broadcasted_iota(jnp.int32, (HEADS, PB, prompt_len), 1).reshape(
            HEADS * PB, prompt_len
        )
        key = lax.broadcasted_iota(jnp.int32, (HEADS * PB, prompt_len), 1)
        out, low = attend_block(q, [(k, v, key <= row + (my_row + start))])
        put_heads(attn, start, PB, out)
        at = pl.multiple_of(i * (HEADS * PB), HEADS * PB)
        nl[pl.ds(at, HEADS * PB), :] = three_parts(low)
        return 0

    lax.fori_loop(0, pref_rows // PB, pref_body, 0)

    def resp_body(i, _):
        start = pl.multiple_of(i * RB, RB)
        q = stacked(rq, start, RB)
        k = kv[pl.ds(base, prompt_len), :HD]
        v = kv[pl.ds(base, prompt_len), HD:]
        row = (
            lax.broadcasted_iota(jnp.int32, (HEADS, RB, RMAX), 1).reshape(HEADS * RB, RMAX) + start
        )
        key = lax.broadcasted_iota(jnp.int32, (HEADS * RB, RMAX), 1)
        out, low = attend_block(q, [(k, v, None), (rk[...], rv[...], key <= row)])
        at_row = (
            lax.broadcasted_iota(jnp.int32, (HEADS, RB, HD), 1).reshape(HEADS * RB, HD) + start
        )
        out = jnp.where(at_row < length, out, 0.0)
        put_heads(attn, pl.multiple_of(pref_rows + start, 64), RB, out)
        at = pl.multiple_of((pref_rows + start) * HEADS, 256)
        nl[pl.ds(at, HEADS * RB), :] = three_parts(low)
        return 0

    live_blocks = (length + RB - 1) // RB
    lax.fori_loop(0, live_blocks, resp_body, 0)

    def dead_body(i, _):
        start = pl.multiple_of(pref_rows + i * RB, 64)
        attn[pl.ds(start, RB), :] = jnp.zeros((RB, HEADS * HD), BF16)
        return 0

    lax.fori_loop(live_blocks, RMAX // RB, dead_body, 0)


def bwd_kernel(
    info, pq, rq, kv, rk, rv, attn, nl, mine, theirs, dq_p, dq_r, dkv, drk, drv, acc_p, acc_r
):
    my_base = pl.multiple_of(info[0], 512)
    my_row = info[1]
    base = pl.multiple_of(info[2], 512)
    length = info[3]
    prompt_len = kv.shape[0] // 2
    pref_rows = pq.shape[0]
    acc_p[...] = jnp.zeros(acc_p.shape, F32)
    acc_r[...] = jnp.zeros(acc_r.shape, F32)

    def dout_rows(start, rows, limit):
        both = mine[pl.ds(start, rows), :] + theirs[pl.ds(start, rows), :].astype(F32)
        if limit is not None:
            at = lax.broadcasted_iota(jnp.int32, both.shape, 0)
            both = jnp.where(at < limit, both, 0.0)
        both = both.astype(BF16)
        return jnp.concatenate([both[:, h * HD : (h + 1) * HD] for h in range(HEADS)], 0)

    def block(q, low, do, out, pieces):
        delta = jnp.sum(do.astype(F32) * out.astype(F32), 1, keepdims=True)
        qx = jnp.concatenate([q, low], 1)
        dox = jnp.concatenate([do, three_parts(-delta)], 1)
        dq = jnp.zeros((q.shape[0], HD), F32)
        for k, v, seen, acc, at in pieces:
            count = k.shape[0]
            ones = jnp.ones((count, HD), BF16)
            p = jnp.exp2(nt(jnp.concatenate([k, ones], 1), qx) * C2)
            if seen is not None:
                p = jnp.where(seen, p, 0.0)
            dp = nt(jnp.concatenate([v, ones], 1), dox)
            ds = (p * dp).astype(BF16)
            acc[pl.ds(at, count), :HD] += nn(ds, q)
            acc[pl.ds(at, count), HD:] += nn(p.astype(BF16), do)
            dq += tn(ds, k)
        return dq * SCALE

    def pieces_of(first_key, seen_of):
        size = 512
        out = []
        for n in range(prompt_len // size):
            at = pl.multiple_of(first_key + n * size, size)
            out.append(
                (kv[pl.ds(at, size), :HD], kv[pl.ds(at, size), HD:], seen_of(n * size), acc_p, at)
            )
        return out

    def pref_body(i, _):
        start = pl.multiple_of(i * PB, PB)
        at = pl.multiple_of(i * (HEADS * PB), HEADS * PB)
        lane = lax.broadcasted_iota(jnp.int32, (1, HEADS * PB), 1)
        row = lane % PB + (my_row + start)

        def seen_of(first):
            key = lax.broadcasted_iota(jnp.int32, (512, HEADS * PB), 0) + first
            return key <= row

        dq = block(
            stacked(pq, start, PB),
            nl[pl.ds(at, HEADS * PB), :],
            dout_rows(start, PB, None),
            stacked(attn, start, PB),
            pieces_of(my_base, seen_of),
        )
        put_heads(dq_p, start, PB, dq)
        return 0

    lax.fori_loop(0, pref_rows // PB, pref_body, 0)

    def resp_body(i, _):
        start = pl.multiple_of(i * RB, RB)
        shifted = pl.multiple_of(pref_rows + start, 64)
        at = pl.multiple_of((pref_rows + start) * HEADS, 256)
        lane = lax.broadcasted_iota(jnp.int32, (1, HEADS * RB), 1)
        row = lane % RB + start
        key = lax.broadcasted_iota(jnp.int32, (RMAX, HEADS * RB), 0)
        dq = block(
            stacked(rq, start, RB),
            nl[pl.ds(at, HEADS * RB), :],
            dout_rows(shifted, RB, length - start),
            stacked(attn, shifted, RB),
            pieces_of(base, lambda first: None) + [(rk[...], rv[...], key <= row, acc_r, 0)],
        )
        put_heads(dq_r, start, RB, dq)
        return 0

    live_blocks = (length + RB - 1) // RB
    lax.fori_loop(0, live_blocks, resp_body, 0)

    def dead_body(i, _):
        start = pl.multiple_of(i * RB, RB)
        dq_r[pl.ds(start, RB), :] = jnp.zeros((RB, HEADS * HD), BF16)
        return 0

    lax.fori_loop(live_blocks, RMAX // RB, dead_body, 0)
    dkv[:, :HD] = (acc_p[:, :HD] * SCALE).astype(BF16)
    dkv[:, HD:] = acc_p[:, HD:].astype(BF16)
    drk[...] = (acc_r[:, :HD] * SCALE).astype(BF16)
    drv[...] = acc_r[:, HD:].astype(BF16)


VM = pl.BlockSpec(memory_space=pltpu.VMEM)
SM = pl.BlockSpec(memory_space=pltpu.SMEM)


def shape_of(dims, dtype=BF16):
    return jax.ShapeDtypeStruct(dims, dtype)


def params(mib=48):
    return pltpu.CompilerParams(vmem_limit_bytes=mib * 1024 * 1024)


def cost(flops, moved, exps=0):
    return pl.CostEstimate(flops=flops, bytes_accessed=moved, transcendentals=exps)


def forward(info, pq, rq, near, far, rk, rv):
    rows = pq.shape[0] + rq.shape[0]
    return pl.pallas_call(
        fwd_kernel,
        out_shape=(
            shape_of((rows, pq.shape[1])),
            shape_of((rows * HEADS, HD)),
            shape_of((near.shape[2] * 16, 2 * HD)),
        ),
        in_specs=[SM] + [VM] * 6,
        out_specs=[VM] * 3,
        compiler_params=params(),
        cost_estimate=cost(3_000_000_000, 6_000_000, 5_500_000),
        name="attend",
    )(info, pq, rq, near, far, rk, rv)


def backward(info, pq, rq, kv, rk, rv, attn, nl, mine, theirs):
    return pl.pallas_call(
        bwd_kernel,
        out_shape=(
            shape_of(pq.shape),
            shape_of(rq.shape),
            shape_of(kv.shape),
            shape_of(rk.shape),
            shape_of(rv.shape),
        ),
        in_specs=[SM] + [VM] * 9,
        out_specs=[VM] * 5,
        scratch_shapes=[pltpu.VMEM((kv.shape[0], 2 * HD), F32), pltpu.VMEM((RMAX, 2 * HD), F32)],
        compiler_params=params(),
        cost_estimate=cost(7_000_000_000, 9_000_000, 5_500_000),
        name="attend_back",
    )(info, pq, rq, kv, rk, rv, attn, nl, mine, theirs)


def pick_weight(info, weight, half):
    rows, width = weight.shape[0], weight.shape[1] // 8

    def at(k, info):
        z, a, c = info[7], info[8], info[6]
        if half:
            return c, (z ^ k) * 2 + (1 - a)
        return 0, (z ^ k) * 2 + a

    def copy(info, w, o):
        o[0] = w[...]

    take = rows // 2 if half else rows
    return pl.pallas_call(
        copy,
        out_shape=shape_of((4, take, width)),
        grid_spec=pltpu.PrefetchScalarGridSpec(
            num_scalar_prefetch=1,
            grid=(4,),
            in_specs=[pl.BlockSpec((take, width), at)],
            out_specs=pl.BlockSpec((1, take, width), lambda k, info: (k, 0, 0)),
        ),
        name="pick_half" if half else "pick_own",
    )(info, weight)


def back_project(grads, weight, dtype):
    def kernel(g0, g1, g2, g3, w, o):
        acc = nt(g0[...], w[0])
        for k, g in enumerate((g1, g2, g3)):
            acc += nt(g[...], w[k + 1])
        o[...] = acc.astype(dtype)

    rows, heads_width = grads[0].shape[0], weight.shape[1]
    return pl.pallas_call(
        kernel,
        out_shape=shape_of((rows, heads_width), dtype),
        in_specs=[VM] * 5,
        out_specs=VM,
        compiler_params=params(),
        cost_estimate=cost(2 * rows * heads_width * 2048, 6_000_000),
        name="back_project",
    )(*grads, weight)


def project(attn, attn_x, own, other):
    def kernel(a, b, w, wx, o0, o1, o2, o3):
        for k, o in enumerate((o0, o1, o2, o3)):
            o[...] = (nn(a[...], w[k]) + nn(b[...], wx[k])).astype(o.dtype)

    rows, width = attn.shape[0], own.shape[2]
    return pl.pallas_call(
        kernel,
        out_shape=(shape_of((rows, width), F32),) + (shape_of((rows, width)),) * 3,
        in_specs=[VM] * 4,
        out_specs=[VM] * 4,
        compiler_params=params(),
        cost_estimate=cost(2 * rows * 1024 * 2048, 9_000_000),
        name="project",
    )(attn, attn_x, own, other)


def weight_grad(info, attn, attn_x, grads):
    def kernel(info, a, b, g0, g1, g2, g3, keep, send):
        c = info[6]
        for side, ref in enumerate((a, b)):
            for half in range(2):
                cols = ref[:, half * 256 : (half + 1) * 256]
                for k, g in enumerate((g0, g1, g2, g3)):
                    part = tn(cols, g[...]).astype(BF16)

                    @pl.when(c == half)
                    def _():
                        keep[side, k] = part

                    @pl.when(c != half)
                    def _():
                        send[side, k] = part

    rows = attn.shape[0]
    out = shape_of((2, 4, 256, 512))
    return pl.pallas_call(
        kernel,
        out_shape=(out, out),
        in_specs=[SM] + [VM] * 6,
        out_specs=[VM] * 2,
        compiler_params=params(),
        cost_estimate=cost(2 * rows * 1024 * 2048, 9_000_000),
        name="weight_grad",
    )(info, attn, attn_x, *grads)


def in_column_order(info, own, other):
    def kernel(info, own, other, o):
        z, a = info[7], info[8]
        for n in range(8):
            k = (n // 2) ^ z

            @pl.when(a == n % 2)
            def _():
                o[:, n * 512 : (n + 1) * 512] = own[k]

            @pl.when(a != n % 2)
            def _():
                o[:, n * 512 : (n + 1) * 512] = other[k]

    return pl.pallas_call(
        kernel,
        out_shape=shape_of((own.shape[1], 8 * own.shape[2])),
        in_specs=[SM] + [VM] * 2,
        out_specs=VM,
        name="column_order",
    )(info, own, other)


def in_row_order(info, near, far):
    rows, width = near.shape[1:]

    def place(m, n, info):
        y, xh, c = info[4], info[5], info[6]
        return ((c ^ m) * 4 + (y ^ (n // 2))) * 2 + (xh ^ (n % 2)), 0

    def kernel(info, near, far, o):
        m = pl.program_id(0)

        @pl.when(m == 0)
        def _():
            o[...] = near[0].astype(F32)

        @pl.when(m == 1)
        def _():
            o[...] = far[0].astype(F32)

    return pl.pallas_call(
        kernel,
        out_shape=shape_of((16 * rows, width), F32),
        grid_spec=pltpu.PrefetchScalarGridSpec(
            num_scalar_prefetch=1,
            grid=(2, 8),
            in_specs=[
                pl.BlockSpec((1, rows, width), lambda m, n, info: (n + m * (7 - n), 0, 0)),
                pl.BlockSpec((1, rows, width), lambda m, n, info: (n * m, 0, 0)),
            ],
            out_specs=pl.BlockSpec((rows, width), place),
        ),
        name="row_order",
    )(info, near, far)


def swap(x, axis, bit):
    return lax.ppermute(x, axis, [(i, i ^ bit) for i in range(lax.axis_size(axis))])


def piece(x, dim, index, size):
    return lax.dynamic_slice_in_dim(x, index * size, size, dim)


def added(*parts):
    total = parts[0].astype(F32)
    for p in parts[1:]:
        total = total + p.astype(F32)
    return total


def on_device(
    prefix_q,
    prefix_k,
    prefix_v,
    resp_q,
    resp_k,
    resp_v,
    resp_len,
    resp_prompt,
    out_weight,
    prefix_grad,
    resp_grad,
):
    head = lax.axis_index("head")
    group = lax.axis_index("group")
    c = lax.axis_index("seq")
    z, a = head // 2, head % 2
    y, xh = group // 2, group % 2
    shard = prefix_k.shape[0]
    prompt_len = shard * 8
    first = (group * 2 + c) * shard
    my_base = first // prompt_len * prompt_len
    info = jnp.stack(
        [my_base, first - my_base, resp_prompt[0] * prompt_len, resp_len[0], y, xh, c, z, a]
    ).astype(jnp.int32)

    kv_own = jnp.concatenate([prefix_k, prefix_v], 1)
    pair = jnp.stack([kv_own, swap(kv_own, "group", 1)])
    grads0 = jnp.concatenate([prefix_grad, resp_grad], 0)
    weight_send = pick_weight(info, out_weight, True)
    weight_own = pick_weight(info, out_weight, False)
    grads = [grads0] + [swap(grads0, "head", 2 * k) for k in (1, 2, 3)]
    weight_x = swap(weight_send, "head", 1)
    weight_y = swap(weight_x, "seq", 1)
    near = jnp.stack([pair] + [swap(pair, "group", 2 * k) for k in (1, 2, 3)])
    far = swap(near, "seq", 1)
    weight_other = jnp.where(
        c == 0,
        jnp.concatenate([weight_x, weight_y], 1),
        jnp.concatenate([weight_y, weight_x], 1),
    )

    attn, low, kv = forward(info, prefix_q, resp_q, near, far, resp_k, resp_v)
    attn_x = swap(attn, "head", 1)
    dout_send = back_project(grads, weight_other, BF16)
    dout_x = swap(dout_send, "head", 1)
    dout_own = back_project(grads, weight_own, F32)

    keep, send = weight_grad(info, attn, attn_x, grads)
    outs = project(attn, attn_x, weight_own, weight_other)
    got = swap(send, "seq", 1)

    dq_p, dq_r, dkv, d_resp_k, d_resp_v = backward(
        info, prefix_q, resp_q, kv, resp_k, resp_v, attn, low, dout_own, dout_x
    )

    out = added(outs[0], *[swap(outs[k], "head", 2 * k) for k in (1, 2, 3)]).astype(BF16)

    def over_y(parts, dim, size):
        sums = [added(*[piece(p, dim, y ^ k, size) for p in parts]) for k in range(4)]
        return [sums[0]] + [swap(sums[k].astype(BF16), "group", 2 * k) for k in (1, 2, 3)]

    parts = over_y((keep, got), 2, 64)
    sent = added(*[piece(p, 2, 1 - xh, 32) for p in parts]).astype(BF16)
    kept = added(*[piece(p, 2, xh, 32) for p in parts])
    block = (kept + swap(sent, "group", 1).astype(F32)).astype(BF16)
    rows_own = in_column_order(info, block[0], swap(block[1], "head", 1))
    rows_two = jnp.stack([rows_own, swap(rows_own, "group", 1)])
    rows_near = jnp.concatenate([rows_two] + [swap(rows_two, "group", 2 * k) for k in (1, 2, 3)], 0)
    rows_far = swap(rows_near, "seq", 1)
    d_out_weight = in_row_order(info, rows_near, rows_far)

    by_core = dkv.reshape(8, 2, shard, 2 * HD)
    core_got = swap(piece(by_core, 1, 1 - c, 1), "seq", 1)
    core_kept = piece(by_core, 1, c, 1)
    kv_parts = over_y((core_kept, core_got), 0, 2)
    kv_sent = added(*[piece(p, 0, 1 - xh, 1) for p in kv_parts]).astype(BF16)
    kv_kept = added(*[piece(p, 0, xh, 1) for p in kv_parts])
    d_prefix = (kv_kept + swap(kv_sent, "group", 1).astype(F32)).astype(BF16).reshape(shard, 2 * HD)
    rows = prefix_q.shape[0]
    return (
        out[:rows],
        out[rows:],
        dq_p,
        d_prefix[:, :HD],
        d_prefix[:, HD:],
        dq_r,
        d_resp_k,
        d_resp_v,
        d_out_weight,
    )


def solution(mesh):
    rows = P(("group", "seq"), "head")
    scalars = P(("group", "seq"))
    in_specs = (rows,) * 6 + (scalars, scalars, P("head", None), rows, rows)
    out_specs = (rows,) * 8 + (P("head", None),)
    return jax.shard_map(
        on_device, mesh=mesh, in_specs=in_specs, out_specs=out_specs, check_vma=False
    )
```

```python
import jax
import jax.numpy as jnp
from jax import lax
from jax.experimental import pallas as pl
from jax.experimental.pallas import tpu as pltpu
from jax.sharding import PartitionSpec as P


HD = 128
RMAX = 512
HEADS = 4
SCALE = HD ** -0.5
C2 = SCALE * 1.4426950408889634
MASKED = -1e30
RB = 128
PB = 96
F32 = jnp.float32
BF16 = jnp.bfloat16


def nt(a, b):
    return lax.dot_general(a, b, (((1,), (1,)), ((), ())), preferred_element_type=F32)


def nn(a, b):
    return jnp.dot(a, b, preferred_element_type=F32)


def tn(a, b):
    return lax.dot_general(a, b, (((0,), (0,)), ((), ())), preferred_element_type=F32)


def stacked(ref, start, rows):
    return jnp.concatenate(
        [ref[pl.ds(start, rows), h * HD : (h + 1) * HD] for h in range(HEADS)], 0
    )


def three_parts(column):
    hi = column.astype(BF16)
    rest = column - hi.astype(F32)
    mid = rest.astype(BF16)
    low = (rest - mid.astype(F32)).astype(BF16)
    lane = lax.broadcasted_iota(jnp.int32, (column.shape[0], HD), 1)
    out = jnp.where(lane == 2, low.astype(F32), 0.0)
    out = jnp.where(lane == 1, mid.astype(F32), out)
    out = jnp.where(lane == 0, hi.astype(F32), out)
    return out.astype(BF16)


def attend_block(q, pieces):
    scores = []
    for k, _, seen in pieces:
        s = nt(q, k)
        if seen is not None:
            s = jnp.where(seen, s, MASKED)
        scores.append(s)
    top = jnp.max(scores[0], 1, keepdims=True)
    for s in scores[1:]:
        top = jnp.maximum(top, jnp.max(s, 1, keepdims=True))
    acc = jnp.zeros((q.shape[0], 2 * HD), F32)
    for s, (_, v, _) in zip(scores, pieces):
        p = jnp.exp2((s - top) * C2).astype(BF16)
        acc += nn(p, jnp.concatenate([v, jnp.ones(v.shape, BF16)], 1))
    total = acc[:, HD : HD + 1]
    out = acc[:, :HD] / total
    return out, -(top + jnp.log(total) * (1.0 / SCALE))


def put_heads(out_ref, start, rows, out):
    for h in range(HEADS):
        out_ref[pl.ds(start, rows), h * HD : (h + 1) * HD] = out[h * rows : (h + 1) * rows].astype(
            BF16
        )


def fwd_kernel(info, pq, rq, near, far, rk, rv, attn, nl, kv):
    my_base = pl.multiple_of(info[0], 512)
    my_row = info[1]
    base = pl.multiple_of(info[2], 512)
    length = info[3]
    y, xh, c = info[4], info[5], info[6]
    shard = near.shape[2]
    prompt_len = kv.shape[0] // 2
    pref_rows = pq.shape[0]
    for m, ref in enumerate((near, far)):
        for k in range(4):
            for j in range(2):
                at = ((y ^ k) * 2 + (xh ^ j)) * 2 + (c ^ m)
                kv[pl.ds(pl.multiple_of(at * shard, shard), shard), :] = ref[k, j]

    def pref_body(i, _):
        start = pl.multiple_of(i * PB, PB)
        q = stacked(pq, start, PB)
        k = kv[pl.ds(my_base, prompt_len), :HD]
        v = kv[pl.ds(my_base, prompt_len), HD:]
        row = lax.broadcasted_iota(jnp.int32, (HEADS, PB, prompt_len), 1).reshape(
            HEADS * PB, prompt_len
        )
        key = lax.broadcasted_iota(jnp.int32, (HEADS * PB, prompt_len), 1)
        out, low = attend_block(q, [(k, v, key <= row + (my_row + start))])
        put_heads(attn, start, PB, out)
        at = pl.multiple_of(i * (HEADS * PB), HEADS * PB)
        nl[pl.ds(at, HEADS * PB), :] = three_parts(low)
        return 0

    lax.fori_loop(0, pref_rows // PB, pref_body, 0)

    def resp_body(i, _):
        start = pl.multiple_of(i * RB, RB)
        q = stacked(rq, start, RB)
        k = kv[pl.ds(base, prompt_len), :HD]
        v = kv[pl.ds(base, prompt_len), HD:]
        row = (
            lax.broadcasted_iota(jnp.int32, (HEADS, RB, RMAX), 1).reshape(HEADS * RB, RMAX) + start
        )
        key = lax.broadcasted_iota(jnp.int32, (HEADS * RB, RMAX), 1)
        out, low = attend_block(q, [(k, v, None), (rk[...], rv[...], key <= row)])
        at_row = (
            lax.broadcasted_iota(jnp.int32, (HEADS, RB, HD), 1).reshape(HEADS * RB, HD) + start
        )
        out = jnp.where(at_row < length, out, 0.0)
        put_heads(attn, pl.multiple_of(pref_rows + start, 64), RB, out)
        at = pl.multiple_of((pref_rows + start) * HEADS, 256)
        nl[pl.ds(at, HEADS * RB), :] = three_parts(low)
        return 0

    live_blocks = (length + RB - 1) // RB
    lax.fori_loop(0, live_blocks, resp_body, 0)

    def dead_body(i, _):
        start = pl.multiple_of(pref_rows + i * RB, 64)
        attn[pl.ds(start, RB), :] = jnp.zeros((RB, HEADS * HD), BF16)
        return 0

    lax.fori_loop(live_blocks, RMAX // RB, dead_body, 0)


def bwd_kernel(
    info,
    pq,
    rq,
    kv,
    rk,
    rv,
    attn,
    nl,
    mine,
    theirs,
    after,
    dq_p,
    dq_r,
    kept,
    sent,
    drk,
    drv,
    acc_p,
    acc_r,
):
    my_base = pl.multiple_of(info[0], 512)
    my_row = info[1]
    base = pl.multiple_of(info[2], 512)
    length = info[3]
    prompt_len = kv.shape[0] // 2
    pref_rows = pq.shape[0]
    acc_p[...] = jnp.zeros(acc_p.shape, F32)
    acc_r[...] = jnp.zeros(acc_r.shape, F32)

    def dout_rows(start, rows, limit):
        both = mine[pl.ds(start, rows), :] + theirs[pl.ds(start, rows), :].astype(F32)
        if limit is not None:
            at = lax.broadcasted_iota(jnp.int32, both.shape, 0)
            both = jnp.where(at < limit, both, 0.0)
        both = both.astype(BF16)
        return jnp.concatenate([both[:, h * HD : (h + 1) * HD] for h in range(HEADS)], 0)

    def block(q, low, do, out, pieces):
        delta = jnp.sum(do.astype(F32) * out.astype(F32), 1, keepdims=True)
        qx = jnp.concatenate([q, low], 1)
        dox = jnp.concatenate([do, three_parts(-delta)], 1)
        dq = jnp.zeros((q.shape[0], HD), F32)
        for k, v, seen, acc, at in pieces:
            count = k.shape[0]
            ones = jnp.ones((count, HD), BF16)
            p = jnp.exp2(nt(jnp.concatenate([k, ones], 1), qx) * C2)
            if seen is not None:
                p = jnp.where(seen, p, 0.0)
            dp = nt(jnp.concatenate([v, ones], 1), dox)
            ds = (p * dp).astype(BF16)
            acc[pl.ds(at, count), :HD] += nn(ds, q)
            acc[pl.ds(at, count), HD:] += nn(p.astype(BF16), do)
            dq += tn(ds, k)
        return dq * SCALE

    def pieces_of(first_key, seen_of):
        size = 512
        out = []
        for n in range(prompt_len // size):
            at = pl.multiple_of(first_key + n * size, size)
            out.append(
                (kv[pl.ds(at, size), :HD], kv[pl.ds(at, size), HD:], seen_of(n * size), acc_p, at)
            )
        return out

    def pref_body(i, _):
        start = pl.multiple_of(i * PB, PB)
        at = pl.multiple_of(i * (HEADS * PB), HEADS * PB)
        lane = lax.broadcasted_iota(jnp.int32, (1, HEADS * PB), 1)
        row = lane % PB + (my_row + start)

        def seen_of(first):
            key = lax.broadcasted_iota(jnp.int32, (512, HEADS * PB), 0) + first
            return key <= row

        dq = block(
            stacked(pq, start, PB),
            nl[pl.ds(at, HEADS * PB), :],
            dout_rows(start, PB, None),
            stacked(attn, start, PB),
            pieces_of(my_base, seen_of),
        )
        put_heads(dq_p, start, PB, dq)
        return 0

    lax.fori_loop(0, pref_rows // PB, pref_body, 0)

    def resp_body(i, _):
        start = pl.multiple_of(i * RB, RB)
        shifted = pl.multiple_of(pref_rows + start, 64)
        at = pl.multiple_of((pref_rows + start) * HEADS, 256)
        lane = lax.broadcasted_iota(jnp.int32, (1, HEADS * RB), 1)
        row = lane % RB + start
        key = lax.broadcasted_iota(jnp.int32, (RMAX, HEADS * RB), 0)
        dq = block(
            stacked(rq, start, RB),
            nl[pl.ds(at, HEADS * RB), :],
            dout_rows(shifted, RB, length - start),
            stacked(attn, shifted, RB),
            pieces_of(base, lambda first: None) + [(rk[...], rv[...], key <= row, acc_r, 0)],
        )
        put_heads(dq_r, start, RB, dq)
        return 0

    live_blocks = (length + RB - 1) // RB
    lax.fori_loop(0, live_blocks, resp_body, 0)

    def dead_body(i, _):
        start = pl.multiple_of(i * RB, RB)
        dq_r[pl.ds(start, RB), :] = jnp.zeros((RB, HEADS * HD), BF16)
        return 0

    lax.fori_loop(live_blocks, RMAX // RB, dead_body, 0)
    shard = kept.shape[1]
    for n in range(kept.shape[0]):
        for m, ref in enumerate((sent, kept)):
            at = (2 * n + (info[6] ^ (1 - m))) * shard
            part = acc_p[pl.ds(pl.multiple_of(at, shard), shard), :]
            ref[n, :, :HD] = (part[:, :HD] * SCALE).astype(BF16)
            ref[n, :, HD:] = part[:, HD:].astype(BF16)
    drk[...] = (acc_r[:, :HD] * SCALE).astype(BF16)
    drv[...] = acc_r[:, HD:].astype(BF16)


VM = pl.BlockSpec(memory_space=pltpu.VMEM)
SM = pl.BlockSpec(memory_space=pltpu.SMEM)
ANY = pl.BlockSpec(memory_space=pl.ANY)
HBM = pl.BlockSpec(memory_space=pltpu.HBM)


def shape_of(dims, dtype=BF16):
    return jax.ShapeDtypeStruct(dims, dtype)


def params(mib=48):
    return pltpu.CompilerParams(vmem_limit_bytes=mib * 1024 * 1024)


def cost(flops, moved, exps=0):
    return pl.CostEstimate(flops=flops, bytes_accessed=moved, transcendentals=exps)


def forward(info, pq, rq, near, far, rk, rv):
    rows = pq.shape[0] + rq.shape[0]
    return pl.pallas_call(
        fwd_kernel,
        out_shape=(
            shape_of((rows, pq.shape[1])),
            shape_of((rows * HEADS, HD)),
            shape_of((near.shape[2] * 16, 2 * HD)),
        ),
        in_specs=[SM] + [VM] * 6,
        out_specs=[VM] * 3,
        compiler_params=params(28),
        cost_estimate=cost(3_000_000_000, 6_000_000, 5_500_000),
        name="attend",
    )(info, pq, rq, near, far, rk, rv)


def backward(info, pq, rq, kv, rk, rv, attn, nl, mine, theirs, after):
    return pl.pallas_call(
        bwd_kernel,
        out_shape=(
            shape_of(pq.shape),
            shape_of(rq.shape),
            shape_of((8, kv.shape[0] // 16, 2 * HD)),
            shape_of((8, kv.shape[0] // 16, 2 * HD)),
            shape_of(rk.shape),
            shape_of(rv.shape),
        ),
        in_specs=[SM] + [VM] * 9 + [ANY],
        out_specs=[VM] * 6,
        scratch_shapes=[pltpu.VMEM((kv.shape[0], 2 * HD), F32), pltpu.VMEM((RMAX, 2 * HD), F32)],
        compiler_params=params(32),
        cost_estimate=cost(7_000_000_000, 9_000_000, 5_500_000),
        name="attend_back",
    )(info, pq, rq, kv, rk, rv, attn, nl, mine, theirs, after)


def pick_half(info, weight):
    rows, width = weight.shape[0] // 2, weight.shape[1] // 8

    def kernel(info, w, o, sems):
        z, a, c = info[7], info[8], info[6]
        copies = []
        for k in range(4):
            block = (z ^ k) * 2 + (1 - a)
            copies.append(
                pltpu.make_async_copy(
                    w.at[
                        pl.ds(pl.multiple_of(c * rows, rows), rows),
                        pl.ds(pl.multiple_of(block * width, width), width),
                    ],
                    o.at[k],
                    sems.at[k],
                )
            )
        for copy in copies:
            copy.start()
        for copy in copies:
            copy.wait()

    return pl.pallas_call(
        kernel,
        out_shape=shape_of((4, rows, width)),
        in_specs=[SM, HBM],
        out_specs=VM,
        scratch_shapes=[pltpu.SemaphoreType.DMA((4,))],
        compiler_params=params(59),
        name="pick_half",
    )(info, weight)


def joined(first, second, dim):
    dims = list(first.shape)
    dims[dim] += second.shape[dim]
    cut = first.shape[dim]

    def kernel(a, b, o, sems):
        if dim == 0:
            places = (o.at[pl.ds(0, cut), :], o.at[pl.ds(cut, dims[0] - cut), :])
        else:
            places = (o.at[:, pl.ds(0, cut)], o.at[:, pl.ds(cut, dims[1] - cut)])
        copies = [
            pltpu.make_async_copy(src, dst, sems.at[n])
            for n, (src, dst) in enumerate(zip((a, b), places))
        ]
        for copy in copies:
            copy.start()
        for copy in copies:
            copy.wait()

    return pl.pallas_call(
        kernel,
        out_shape=shape_of(tuple(dims)),
        in_specs=[ANY] * 2,
        out_specs=VM,
        scratch_shapes=[pltpu.SemaphoreType.DMA((2,))],
        compiler_params=params(60),
    )(first, second)


def own_block(info, w, k):
    z, a = info[7], info[8]
    width = w.shape[1] // 8
    block = (z ^ k) * 2 + a
    return w[:, pl.ds(pl.multiple_of(block * width, width), width)]


def back_project_other(info, grads, weight_x, weight_c, after):
    def kernel(info, g0, g1, g2, g3, wx, wc, after, o):
        c = info[6]
        sums = []
        for w in (wx, wc):
            acc = nt(g0[...], w[0])
            for k, g in enumerate((g1, g2, g3)):
                acc += nt(g[...], w[k + 1])
            sums.append(acc.astype(BF16))
        width = o.shape[1] // 2
        for half in range(2):

            @pl.when(c == half)
            def _():
                o[:, half * width : (half + 1) * width] = sums[0]
                o[:, (1 - half) * width : (2 - half) * width] = sums[1]

    rows = grads[0].shape[0]
    width = 2 * weight_x.shape[1]
    return pl.pallas_call(
        kernel,
        out_shape=shape_of((rows, width)),
        in_specs=[SM] + [VM] * 6 + [ANY],
        out_specs=VM,
        compiler_params=params(16),
        cost_estimate=cost(2 * rows * width * 2048, 6_000_000),
        name="back_other",
    )(info, *grads, weight_x, weight_c, after)


def back_project_own(info, grads, weight, after):
    def kernel(info, g0, g1, g2, g3, w, after, o):
        acc = nt(g0[...], own_block(info, w, 0))
        for k, g in enumerate((g1, g2, g3)):
            acc += nt(g[...], own_block(info, w, k + 1))
        o[...] = acc

    rows = grads[0].shape[0]
    return pl.pallas_call(
        kernel,
        out_shape=shape_of((rows, weight.shape[0]), F32),
        in_specs=[SM] + [VM] * 5 + [ANY],
        out_specs=VM,
        compiler_params=params(18),
        cost_estimate=cost(2 * rows * weight.shape[0] * 2048, 8_000_000),
        name="back_own",
    )(info, *grads, weight, after)


def project(info, attn, attn_x, weight, weight_x, weight_c, after):
    def kernel(info, a, b, w, wx, wc, after, o0, o1, o2, o3):
        c = info[6]
        half = wx.shape[1]
        b_same = b[:, pl.ds(pl.multiple_of(c * half, half), half)]
        b_flip = b[:, pl.ds(pl.multiple_of((1 - c) * half, half), half)]
        part = (nn(a[...], w[...]) + nn(b_same, wx[0]) + nn(b_flip, wc[0])).astype(BF16)
        for n, o in enumerate((o1, o2, o3, o0)):

            @pl.when(pl.program_id(0) == n)
            def _():
                o[...] = part

    rows, width = attn.shape[0], weight.shape[1] // 8
    whole = pl.BlockSpec((rows, width), lambda n, info: (0, 0))
    half = pl.BlockSpec((1, weight.shape[0] // 2, width), lambda n, info: ((n + 1) % 4, 0, 0))
    own = pl.BlockSpec(
        (weight.shape[0], width), lambda n, info: (0, (info[7] ^ ((n + 1) % 4)) * 2 + info[8])
    )
    return pl.pallas_call(
        kernel,
        out_shape=(shape_of((rows, width)),) * 4,
        grid_spec=pltpu.PrefetchScalarGridSpec(
            num_scalar_prefetch=1,
            grid=(4,),
            in_specs=[whole, whole, own, half, half, ANY],
            out_specs=[whole] * 4,
        ),
        compiler_params=params(52),
        cost_estimate=cost(2 * rows * 1024 * 2048, 9_000_000),
        name="project",
    )(info, attn, attn_x, weight, weight_x, weight_c, after)


def out_sum(parts, cut):
    rows, width = parts[0].shape

    def kernel(p0, p1, p2, p3, o, q):
        for ref, at in ((o, pl.ds(0, cut)), (q, pl.ds(cut, rows - cut))):
            total = p0[at, :].astype(F32) + p1[at, :].astype(F32)
            total += p2[at, :].astype(F32) + p3[at, :].astype(F32)
            ref[...] = total.astype(BF16)

    def whole(count):
        return pl.BlockSpec((count, width), lambda n: (0, 0))

    return pl.pallas_call(
        kernel,
        out_shape=(shape_of((cut, width)), shape_of((rows - cut, width))),
        grid=(1,),
        in_specs=[whole(rows)] * 4,
        out_specs=[whole(cut), whole(rows - cut)],
        compiler_params=params(44),
        cost_estimate=cost(2_000_000_000, 5_000_000),
        name="out_sum",
    )(*parts)


def weight_grad(info, attn, grads, after):
    def kernel(info, a, g0, g1, g2, g3, after, keep, send):
        c = info[6]
        for k, g in enumerate((g0, g1, g2, g3)):
            part = tn(a[...], g[...]).astype(BF16)
            for half in range(2):
                rows = part[half * 256 : (half + 1) * 256]

                @pl.when(c == half)
                def _():
                    keep[k] = rows

                @pl.when(c != half)
                def _():
                    send[k] = rows

    rows = attn.shape[0]
    out = shape_of((4, 256, 512))
    return pl.pallas_call(
        kernel,
        out_shape=(out, out),
        in_specs=[SM] + [VM] * 5 + [ANY],
        out_specs=[VM] * 2,
        compiler_params=params(16),
        cost_estimate=cost(2 * rows * 512 * 2048, 7_000_000),
    )(info, attn, *grads, after)


def assemble(info, parts):
    rows = parts[0].shape[1]

    def kernel(info, p0, p1, p2, p3, o):
        y = info[4]
        for k, p in enumerate((p0, p1, p2, p3)):
            o[:, pl.ds(pl.multiple_of((y ^ k) * rows, rows), rows), :] = p[...]

    return pl.pallas_call(
        kernel,
        out_shape=shape_of((4, 4 * rows, parts[0].shape[2])),
        in_specs=[SM] + [VM] * 4,
        out_specs=VM,
        compiler_params=params(8),
    )(info, *parts)


def widen(info, sources, side, before):
    blocks, rows, width = sources[0][0].shape
    count = len(sources)

    def kernel(info, *refs):
        c, z, a = info[6], info[7], info[8]
        wide, sems = refs[-2:]
        o = refs[-3]
        copies = []
        for n, (_, far) in enumerate(sources):
            for k in range(blocks):
                slot = n * blocks + k
                wide[slot] = refs[n][k].astype(F32)
                row = pl.multiple_of((c ^ far) * rows, rows)
                col = pl.multiple_of(((z ^ k) * 2 + (a ^ side)) * width, width)
                copy = pltpu.make_async_copy(
                    wide.at[slot], o.at[pl.ds(row, rows), pl.ds(col, width)], sems.at[slot]
                )
                copy.start()
                copies.append(copy)
        for copy in copies:
            copy.wait()

    return pl.pallas_call(
        kernel,
        out_shape=shape_of((2 * rows, 2 * blocks * width), F32),
        in_specs=[SM] + [VM] * count + ([] if before is None else [HBM]),
        out_specs=HBM,
        scratch_shapes=[
            pltpu.VMEM((count * blocks, rows, width), F32),
            pltpu.SemaphoreType.DMA((count * blocks,)),
        ],
        input_output_aliases={} if before is None else {1 + count: 0},
        compiler_params=params(12),
        cost_estimate=cost(1_000_000_000 * count, 4_000_000 * count),
    )(info, *[x for x, _ in sources], *([] if before is None else [before]))


def split_sum(info, keep, got):
    blocks, rows, width = keep.shape
    size = rows // 4

    def kernel(info, a, b, o0, o1, o2, o3):
        y = info[4]
        for k in (1, 3, 2, 0):
            o = (o0, o1, o2, o3)[k]
            at = pl.ds(pl.multiple_of((y ^ k) * size, size), size)
            o[...] = (a[:, at, :].astype(F32) + b[:, at, :].astype(F32)).astype(o.dtype)

    return pl.pallas_call(
        kernel,
        out_shape=(shape_of((blocks, size, width), F32),)
        + (shape_of((blocks, size, width)),) * 3,
        in_specs=[SM] + [VM] * 2,
        out_specs=[VM] * 4,
        compiler_params=params(10),
        cost_estimate=cost(1_000_000_000, 3_000_000),
    )(info, keep, got)


def split_keys(info, keep, got):
    pairs, rows, width = keep.shape

    def kernel(info, a, b, o0, o1, o2, o3):
        y = info[4]
        for k in (1, 3, 2, 0):
            o = (o0, o1, o2, o3)[k]
            for j in range(2):
                at = (y ^ k) * 2 + j
                o[j] = (a[at].astype(F32) + b[at].astype(F32)).astype(o.dtype)

    out = (pairs // 4, rows, width)
    return pl.pallas_call(
        kernel,
        out_shape=(shape_of(out, F32),) + (shape_of(out),) * 3,
        in_specs=[SM] + [VM] * 2,
        out_specs=[VM] * 4,
        compiler_params=params(10),
        cost_estimate=cost(1_000_000_000, 3_000_000),
        name="split_keys",
    )(info, keep, got)


def swap(x, axis, bit):
    return lax.ppermute(x, axis, [(i, i ^ bit) for i in range(lax.axis_size(axis))])


def piece(x, dim, index, size):
    return lax.dynamic_slice_in_dim(x, index * size, size, dim)


def added(*parts):
    total = parts[0].astype(F32)
    for p in parts[1:]:
        total = total + p.astype(F32)
    return total


def on_device(
    prefix_q,
    prefix_k,
    prefix_v,
    resp_q,
    resp_k,
    resp_v,
    resp_len,
    resp_prompt,
    out_weight,
    prefix_grad,
    resp_grad,
):
    head = lax.axis_index("head")
    group = lax.axis_index("group")
    c = lax.axis_index("seq")
    z, a = head // 2, head % 2
    y, xh = group // 2, group % 2
    shard = prefix_k.shape[0]
    prompt_len = shard * 8
    first = (group * 2 + c) * shard
    my_base = first // prompt_len * prompt_len
    info = jnp.stack(
        [my_base, first - my_base, resp_prompt[0] * prompt_len, resp_len[0], y, xh, c, z, a]
    ).astype(jnp.int32)

    def over_y(parts):
        return [parts[0]] + [swap(parts[k], "group", 2 * k) for k in (1, 2, 3)]

    kv_own = joined(prefix_k, prefix_v, 1)
    pair = jnp.stack([kv_own, swap(kv_own, "group", 1)])
    grads0 = joined(prefix_grad, resp_grad, 0)
    grads = [grads0] + [swap(grads0, "head", 2 * k) for k in (1, 2, 3)]
    near = jnp.stack(over_y([pair] * 4))
    far = swap(near, "seq", 1)
    weight_send = pick_half(info, out_weight)
    weight_x = swap(weight_send, "head", 1)
    weight_c = swap(weight_x, "seq", 1)

    attn, low, kv = forward(info, prefix_q, resp_q, near, far, resp_k, resp_v)
    attn_x = swap(attn, "head", 1)
    keep_a, send_a = weight_grad(info, attn, grads, low)
    got_a = swap(send_a, "seq", 1)
    dout_send = back_project_other(info, grads, weight_x, weight_c, keep_a)
    dout_x = swap(dout_send, "head", 1)
    dout_own = back_project_own(info, grads, out_weight, dout_send)
    parts_a = over_y(split_sum(info, keep_a, got_a))
    keep_b, send_b = weight_grad(info, attn_x, grads, dout_own)
    got_b = swap(send_b, "seq", 1)
    outs = project(info, attn, attn_x, out_weight, weight_x, weight_c, keep_b)
    out_parts = [outs[0]] + [swap(outs[k], "head", 2 * k) for k in (1, 2, 3)]
    parts_b = over_y(split_sum(info, keep_b, got_b))
    dq_p, dq_r, dk_kept, dk_sent, d_resp_k, d_resp_v = backward(
        info, prefix_q, resp_q, kv, resp_k, resp_v, attn, low, dout_own, dout_x, outs[1]
    )
    rows = prefix_q.shape[0]
    prefix_out, resp_out = out_sum(out_parts, rows)

    y_sum_a = added(*parts_a).astype(BF16)
    block_a = added(y_sum_a, swap(y_sum_a, "group", 1)).astype(BF16)
    half_a = assemble(info, over_y([block_a] * 4))
    grad = widen(info, [(half_a, 0), (swap(half_a, "seq", 1), 1)], 0, None)

    y_sum_b = added(*parts_b).astype(BF16)
    across = lax.ppermute(
        y_sum_b,
        ("group", "head"),
        [(g * 8 + h, (g ^ 1) * 8 + (h ^ 1)) for g in range(8) for h in range(8)],
    )
    block_b = added(swap(y_sum_b, "head", 1), across).astype(BF16)
    half_b = assemble(info, over_y([block_b] * 4))
    grad = widen(info, [(half_b, 0)], 1, grad)
    grad = widen(info, [(swap(half_b, "seq", 1), 1)], 1, grad)

    got_k = swap(dk_sent, "seq", 1)
    parts_k = over_y(split_keys(info, dk_kept, got_k))
    sent_k = added(*[piece(p, 0, 1 - xh, 1) for p in parts_k]).astype(BF16)
    kept_k = added(*[piece(p, 0, xh, 1) for p in parts_k])
    d_prefix = (kept_k + swap(sent_k, "group", 1).astype(F32)).astype(BF16)
    d_prefix = d_prefix.reshape(shard, 2 * HD)
    return (
        prefix_out,
        resp_out,
        dq_p,
        d_prefix[:, :HD],
        d_prefix[:, HD:],
        dq_r,
        d_resp_k,
        d_resp_v,
        grad,
    )


def solution(mesh):
    rows = P(("group", "seq"), "head")
    scalars = P(("group", "seq"))
    in_specs = (rows,) * 6 + (scalars, scalars, P("head", None), rows, rows)
    out_specs = (rows,) * 8 + (P("head", None),)

    def step(*args):
        return on_device(*args)

    step = jax.shard_map(step, mesh=mesh, in_specs=in_specs, out_specs=out_specs, check_vma=False)
    return step
```
